64 devices in a mesh: dp: 4 (over x, y), tp: 16 (over z, core).
Axes of the slice: x: 2, y: 2, z: 8, core: 2. Of those that a mesh axis runs over, the one named last changes fastest.
The devices are a block of a 4x4x8 slice.
Arguments:
- x: bfloat16 [512, 2048], P('dp'), parts along dimension 0
- lengths: int32 [512], P('dp'), parts along dimension 0
- k_cache: bfloat16 [2, 512, 128, 16, 128], P(None, 'dp', None, 'tp'), parts along dimension 1
- v_cache: bfloat16 [2, 512, 128, 16, 128], P(None, 'dp', None, 'tp'), parts along dimension 1
- attn_norm: float32 [2, 2048], replicated
- mlp_norm: float32 [2, 2048], replicated
- w_q: bfloat16 [2, 2048, 2048], P(None, None, 'tp')
- w_k: bfloat16 [2, 2048, 2048], P(None, None, 'tp')
- w_v: bfloat16 [2, 2048, 2048], P(None, None, 'tp')
- w_o: bfloat16 [2, 2048, 2048], P(None, 'tp')
- w_gate: bfloat16 [2, 2048, 8192], P(None, None, 'tp')
- w_up: bfloat16 [2, 2048, 8192], P(None, None, 'tp')
- w_down: bfloat16 [2, 8192, 2048], P(None, 'tp')
Outputs:
- output: bfloat16 [512, 2048], P('dp'), parts along dimension 0
There are 4 independent parts. The reference program is written for one: setup_inputs(seed, part) draws one part's arguments, and reference() takes and returns one part's arrays. A program takes and returns all parts, laid end to end along the dimension named above; an argument that names none is the same for every part.
All inputs are finite; a program needn't handle non-finite values.
Results may differ from the reference program's by a relative error of at most 0.02.
Values are sent between devices in bfloat16 or wider.
A program may use at most 768 MiB of HBM per device.

```python
import jax
import jax.numpy as jnp
from jax import lax

D = 2048
HEADS = 16
KV_HEADS = 16
HEAD = 128
FF = 8192
BATCH = 128
SEQ = 128
TP = 16
LAYERS = 2
NORM_EPS = 1e-5
ROPE_BASE = 10000.0
Q_GAIN = 2.5
OUT_GAIN = 1.5


def draw_normal(rng_key, arr_shape, factor):
    return (jax.random.normal(rng_key, arr_shape, jnp.float32) * factor).astype(jnp.bfloat16)


def setup_inputs(seed: int = 0, part: int = 0) -> dict:
    shared_keys = jax.random.split(jax.random.key(seed), 9)
    part_keys = jax.random.split(jax.random.fold_in(jax.random.key(seed + 1), part), 4)
    width_q = HEADS * HEAD
    width_kv = KV_HEADS * HEAD
    cache_shape = (LAYERS, BATCH, SEQ, KV_HEADS, HEAD)
    lengths = jax.random.randint(part_keys[3], (BATCH,), 1, SEQ, dtype=jnp.int32)
    lengths = lengths.at[0].set(SEQ - 1).at[BATCH - 1].set(1)
    return {
        "x": draw_normal(part_keys[0], (BATCH, D), 1.0),
        "lengths": lengths,
        "k_cache": draw_normal(part_keys[1], cache_shape, 1.0),
        "v_cache": draw_normal(part_keys[2], cache_shape, 1.0),
        "attn_norm": jax.random.uniform(shared_keys[0], (LAYERS, D), jnp.float32, 0.5, 1.5),
        "mlp_norm": jax.random.uniform(shared_keys[1], (LAYERS, D), jnp.float32, 0.5, 1.5),
        "w_q": draw_normal(shared_keys[2], (LAYERS, D, width_q), Q_GAIN * D ** -0.5),
        "w_k": draw_normal(shared_keys[3], (LAYERS, D, width_kv), D ** -0.5),
        "w_v": draw_normal(shared_keys[4], (LAYERS, D, width_kv), D ** -0.5),
        "w_o": draw_normal(shared_keys[5], (LAYERS, width_q, D), OUT_GAIN * width_q ** -0.5),
        "w_gate": draw_normal(shared_keys[6], (LAYERS, D, FF), D ** -0.5),
        "w_up": draw_normal(shared_keys[7], (LAYERS, D, FF), D ** -0.5),
        "w_down": draw_normal(shared_keys[8], (LAYERS, FF, D), OUT_GAIN * FF ** -0.5),
    }


def rms_norm(hidden_in, norm_gain):
    mean_sq = jnp.mean(hidden_in * hidden_in, axis=-1, keepdims=True)
    return (hidden_in * lax.rsqrt(mean_sq + NORM_EPS) * norm_gain).astype(jnp.bfloat16)


def rope_tables(lengths):
    inv_freq = ROPE_BASE ** (-jnp.arange(0, HEAD, 2).astype(jnp.float32) / HEAD)
    angles = lengths.astype(jnp.float32)[:, None] * inv_freq[None, :]
    return jnp.cos(angles)[:, None, :], jnp.sin(angles)[:, None, :]


def apply_rope(proj_out, cos_t, sin_t):
    half_dim = proj_out.shape[-1] // 2
    first_half = proj_out[..., :half_dim]
    second_half = proj_out[..., half_dim:]
    return jnp.concatenate([first_half * cos_t - second_half * sin_t, second_half * cos_t + first_half * sin_t], axis=-1)


def attention(q_heads, k_new, v_new, k_layer, v_layer, lengths):
    batch_n = k_layer.shape[0]
    seq_n = k_layer.shape[1]
    group_n = HEADS // KV_HEADS
    inv_scale = HEAD ** -0.5
    q_group = q_heads.reshape(batch_n, KV_HEADS, group_n, HEAD).astype(jnp.float32)
    logits = jnp.einsum("bkgd,bskd->bkgs", q_group, k_layer.astype(jnp.float32)) * inv_scale
    valid_mask = jnp.arange(seq_n)[None, None, None, :] < lengths[:, None, None, None]
    logits = jnp.where(valid_mask, logits, -1e30)
    logit_new = jnp.einsum("bkgd,bkd->bkg", q_group, k_new.astype(jnp.float32)) * inv_scale
    row_max = jnp.maximum(jnp.max(logits, axis=-1), logit_new)
    prob_cache = jnp.exp(logits - row_max[..., None])
    prob_new = jnp.exp(logit_new - row_max)
    prob_sum = jnp.sum(prob_cache, axis=-1) + prob_new
    weighted = jnp.einsum("bkgs,bskd->bkgd", prob_cache.astype(jnp.bfloat16).astype(jnp.float32), v_layer.astype(jnp.float32))
    weighted = weighted + prob_new.astype(jnp.bfloat16).astype(jnp.float32)[..., None] * v_new.astype(jnp.float32)[:, :, None, :]
    return (weighted / prob_sum[..., None]).astype(jnp.bfloat16).reshape(batch_n, HEADS * HEAD)


def block_sum(activations, weight):
    act_blocks = activations.reshape(activations.shape[0], TP, -1).astype(jnp.float32)
    weight_blocks = weight.reshape(TP, -1, weight.shape[1]).astype(jnp.float32)
    partials = jnp.einsum("btk,tkn->tbn", act_blocks, weight_blocks).astype(jnp.bfloat16)
    return jnp.sum(partials.astype(jnp.float32), axis=0)


def reference(x, lengths, k_cache, v_cache, attn_norm, mlp_norm, w_q, w_k, w_v, w_o, w_gate, w_up, w_down):
    batch_n = x.shape[0]
    cos_t, sin_t = rope_tables(lengths)
    residual = x
    for layer_idx in range(LAYERS):
        resid_f = residual.astype(jnp.float32)
        normed = rms_norm(resid_f, attn_norm[layer_idx])
        q_proj = jnp.dot(normed, w_q[layer_idx], preferred_element_type=jnp.float32)
        k_proj = jnp.dot(normed, w_k[layer_idx], preferred_element_type=jnp.float32)
        q_heads = apply_rope(q_proj.reshape(batch_n, HEADS, HEAD), cos_t, sin_t).astype(jnp.bfloat16)
        k_new = apply_rope(k_proj.reshape(batch_n, KV_HEADS, HEAD), cos_t, sin_t).astype(jnp.bfloat16)
        v_new = jnp.dot(normed, w_v[layer_idx], preferred_element_type=jnp.float32).astype(jnp.bfloat16).reshape(batch_n, KV_HEADS, HEAD)
        attn_out = attention(q_heads, k_new, v_new, k_cache[layer_idx], v_cache[layer_idx], lengths)
        hidden_f = (resid_f + block_sum(attn_out, w_o[layer_idx])).astype(jnp.bfloat16).astype(jnp.float32)
        normed_mlp = rms_norm(hidden_f, mlp_norm[layer_idx])
        gate_proj = jnp.dot(normed_mlp, w_gate[layer_idx], preferred_element_type=jnp.float32)
        up_proj = jnp.dot(normed_mlp, w_up[layer_idx], preferred_element_type=jnp.float32)
        mlp_act = (jax.nn.silu(gate_proj) * up_proj).astype(jnp.bfloat16)
        residual = (hidden_f + block_sum(mlp_act, w_down[layer_idx])).astype(jnp.bfloat16)
    return residual
```

```python
import functools

import jax
import jax.numpy as jnp
import numpy as np
from jax import lax
from jax.experimental import pallas as pl
from jax.experimental.pallas import tpu as pltpu
from jax.sharding import PartitionSpec as P

NORM_EPS = 1e-5
ROPE_BASE = 10000.0
MESH = pl.DeviceIdType.MESH
F32 = jnp.float32
BF16 = jnp.bfloat16


def nt_dot(a, b):
    return lax.dot_general(a, b, (((1,), (1,)), ((), ())), preferred_element_type=F32)


def dot(a, b):
    return jnp.dot(a, b, preferred_element_type=F32)


def kernel(n, x_ref, len_ref, freq_ref, k_ref, v_ref, an_ref, mn_ref, wq_ref, wk_ref, wv_ref, wo_ref, wg_ref, wu_ref, wd_ref,
           out_ref, hid, act, kbuf, vbuf, wqkv, wo, wg, wu, wd, gains, lens, freqs, cosb, sinb, scores, qb, obuf, ubuf, part, recv, own,
           in_sem, x_sem, w_sem, out_sem, a_send, a_recv, g_send, g_recv):
    chips, toks, width = hid.shape
    half = toks // 2
    layers = kbuf.shape[0]
    head = kbuf.shape[-1]
    seq = kbuf.shape[2]
    me = lax.axis_index("tp")
    z, core = me // 2, lax.rem(me, 2)

    def cp(src, dst, sem):
        return pltpu.make_async_copy(src, dst, sem)

    x_copies = [cp(x_ref.at[:, pl.ds(width * t, width)], hid.at[t], x_sem.at[t]) for t in range(chips)]
    small = [cp(len_ref, lens, in_sem.at[0]), cp(freq_ref, freqs, in_sem.at[1]), cp(an_ref, gains.at[0], in_sem.at[2]),
             cp(mn_ref, gains.at[1], in_sem.at[3])]

    def layer_copies(l):
        return [
            cp(wq_ref.at[l], wqkv.at[l, :, pl.ds(0, head)], w_sem.at[l, 0]),
            cp(wk_ref.at[l], wqkv.at[l, :, pl.ds(head, head)], w_sem.at[l, 1]),
            cp(wv_ref.at[l], wqkv.at[l, :, pl.ds(2 * head, head)], w_sem.at[l, 2]),
            cp(k_ref.at[l], kbuf.at[l], w_sem.at[l, 3]),
            cp(v_ref.at[l], vbuf.at[l], w_sem.at[l, 4]),
            cp(wo_ref.at[l], wo.at[l], w_sem.at[l, 5]),
            cp(wg_ref.at[l], wg.at[l], w_sem.at[l, 6]),
            cp(wu_ref.at[l], wu.at[l], w_sem.at[l, 7]),
            cp(wd_ref.at[l], wd.at[l], w_sem.at[l, 8]),
        ]

    for c in x_copies + small:
        c.start()
    for l in range(layers):
        for c in layer_copies(l):
            c.start()

    barrier = pltpu.get_barrier_semaphore()
    for d in range(1, n):
        pl.semaphore_signal(barrier, inc=1, device_id={"tp": lax.rem(me + d, n)}, device_id_type=MESH)

    for c in small:
        c.wait()
    lens_rows = jnp.transpose(jnp.broadcast_to(lens[...].astype(F32), (toks, toks)))
    angle = lens_rows[:, :head] * freqs[...]
    lane = lax.broadcasted_iota(jnp.int32, (toks, head), 1)
    cosb[...] = jnp.cos(angle)
    sinb[...] = jnp.where(lane < head // 2, -1.0, 1.0) * jnp.sin(angle)
    for c in x_copies:
        c.wait()
    own[...] = hid[z, pl.ds(pl.multiple_of(half * core, half), half), :]
    pl.semaphore_wait(barrier, n - 1)

    def norm(which, l):
        total = jnp.zeros((toks, width), F32)
        for t in range(chips):
            h = hid[t].astype(F32)
            total = total + h * h
        inv = lax.rsqrt(jnp.sum(total, axis=1, keepdims=True) / (chips * width) + NORM_EPS)
        for t in range(chips):
            gain = gains[which, pl.ds(l, 1), pl.ds(width * t, width)]
            act[:, pl.ds(width * t, width)] = (hid[t].astype(F32) * inv * gain).astype(BF16)

    def reduce_gather(src_ref, w_ref, l):
        def chip_block(i, _):
            t = lax.rem(z + 4 + i, chips)
            cols = pl.ds(pl.multiple_of(t * width, width), width)
            part[t] = dot(src_ref[...], w_ref[l, :, cols]).astype(BF16)
            return 0

        lax.fori_loop(0, chips, chip_block, 0)

        def exchange(d):
            to = lax.rem(me + d, n)
            rows = pl.ds(pl.multiple_of(half * lax.rem(to, 2), half), half)
            return pltpu.make_async_remote_copy(
                src_ref=part.at[to // 2, rows], dst_ref=recv.at[d - 1], send_sem=a_send.at[d - 1], recv_sem=a_recv.at[d - 1],
                device_id={"tp": to}, device_id_type=MESH)

        for d in range(1, n):
            exchange(d).start()
        mine = pl.ds(pl.multiple_of(half * core, half), half)
        total = part[z, mine, :].astype(F32)
        for d in range(1, n):
            exchange(d).wait()
            total = total + recv[d - 1].astype(F32)
        own[...] = (own[...].astype(F32) + total).astype(BF16)
        hid[z, mine, :] = own[...]

        def gather(d):
            to = lax.rem(me + d, n)
            return pltpu.make_async_remote_copy(
                src_ref=own, dst_ref=hid.at[z, mine], send_sem=g_send.at[d - 1], recv_sem=g_recv.at[d - 1],
                device_id={"tp": to}, device_id_type=MESH)

        for d in range(1, n):
            gather(d).start()
        for d in range(1, n):
            gather(d).wait()

    def layer(l, _):
        norm(0, l)
        copies = layer_copies(l)
        for c in copies[:3]:
            c.wait()
        qkv = dot(act[...], wqkv[l])
        cos, sin = cosb[...], sinb[...]

        def rope(p):
            return (p * cos + pltpu.roll(p, head // 2, 1) * sin).astype(BF16)

        q = rope(qkv[:, :head])
        k_new = rope(qkv[:, head:2 * head])
        v_new = qkv[:, 2 * head:].astype(BF16)
        scale = head ** -0.5
        logit_new = jnp.sum(q.astype(F32) * k_new.astype(F32), axis=1, keepdims=True) * scale
        qb[...] = q
        copies[3].wait()
        step = 16
        row = lax.broadcasted_iota(jnp.int32, (step, seq), 0)

        def qk(i, _):
            rows = pl.ds(pl.multiple_of(i * step, step), step)
            full = nt_dot(qb[rows, :], kbuf[l, rows].reshape(step * seq, head))
            picked = full[:, :seq]
            for j in range(1, step):
                picked = jnp.where(row == j, full[:, j * seq:(j + 1) * seq], picked)
            scores[rows, :] = picked
            return 0

        lax.fori_loop(0, toks // step, qk, 0)
        lens_rows = jnp.transpose(jnp.broadcast_to(lens[...], (toks, toks)))
        lane = lax.broadcasted_iota(jnp.int32, (toks, seq), 1)
        logits = jnp.where(lane < lens_rows, scores[...] * scale, -1e30)
        top = jnp.maximum(jnp.max(logits, axis=1, keepdims=True), logit_new)
        p = jnp.exp(logits - top)
        p_new = jnp.exp(logit_new - top)
        denom = jnp.sum(p, axis=1, keepdims=True) + p_new
        scores[...] = p
        copies[4].wait()

        def pv(i, _):
            rows = pl.ds(pl.multiple_of(i * step, step), step)
            mine = scores[rows, :]
            spread = jnp.concatenate([jnp.where(row == j, mine, 0.0).astype(BF16) for j in range(step)], axis=1)
            scores[rows, :] = dot(spread, vbuf[l, rows].reshape(step * seq, head))
            return 0

        lax.fori_loop(0, toks // step, pv, 0)
        weighted = scores[...] + p_new.astype(BF16).astype(F32) * v_new.astype(F32)
        obuf[...] = (weighted / denom).astype(BF16)
        copies[5].wait()
        reduce_gather(obuf, wo, l)
        norm(1, l)
        copies[6].wait()
        copies[7].wait()
        for t in range(wg.shape[-1] // 256):
            cols = pl.ds(256 * t, 256)
            gate = dot(act[...], wg[l, :, cols])
            up = dot(act[...], wu[l, :, cols])
            ubuf[:, cols] = (jax.nn.silu(gate) * up).astype(BF16)
        copies[8].wait()
        reduce_gather(ubuf, wd, l)
        return 0

    lax.fori_loop(0, layers, layer, 0)
    outs = [cp(hid.at[t], out_ref.at[:, pl.ds(width * t, width)], out_sem.at[t]) for t in range(chips)]
    for c in outs:
        c.start()
    for c in outs:
        c.wait()


def solution(mesh):
    n = mesh.shape["tp"]
    cache_spec = P(None, "dp", None, "tp", None)
    col_spec = P(None, None, "tp")
    row_spec = P(None, "tp", None)
    in_specs = (P("dp", None), P("dp"), cache_spec, cache_spec, P(), P(), col_spec, col_spec, col_spec, row_spec, col_spec, col_spec, row_spec)

    def step(x, lengths, k_cache, v_cache, attn_norm, mlp_norm, w_q, w_k, w_v, w_o, w_gate, w_up, w_down):
        toks, dim = x.shape
        layers, _, seq, _, head = k_cache.shape
        ff = w_gate.shape[2]
        chips = n // 2
        width = dim // chips
        half = toks // 2
        k = k_cache.reshape(layers, toks, seq, head)
        v = v_cache.reshape(layers, toks, seq, head)
        freq = ROPE_BASE ** (-np.arange(0, head, 2, dtype=np.float32) / head)
        freq = jnp.asarray(np.concatenate([freq, freq])[None, :].astype(np.float32))
        dma = pltpu.SemaphoreType.DMA
        scratch = [
            pltpu.VMEM((chips, toks, width), BF16),
            pltpu.VMEM((toks, dim), BF16),
            pltpu.VMEM((layers, toks, seq, head), BF16),
            pltpu.VMEM((layers, toks, seq, head), BF16),
            pltpu.VMEM((layers, dim, 3 * head), BF16),
            pltpu.VMEM((layers, head, dim), BF16),
            pltpu.VMEM((layers, dim, ff), BF16),
            pltpu.VMEM((layers, dim, ff), BF16),
            pltpu.VMEM((layers, ff, dim), BF16),
            pltpu.VMEM((2, layers, dim), F32),
            pltpu.VMEM((1, toks), jnp.int32),
            pltpu.VMEM((1, head), F32),
            pltpu.VMEM((toks, head), F32),
            pltpu.VMEM((toks, head), F32),
            pltpu.VMEM((toks, seq), F32),
            pltpu.VMEM((toks, head), BF16),
            pltpu.VMEM((toks, head), BF16),
            pltpu.VMEM((toks, ff), BF16),
            pltpu.VMEM((chips, toks, width), BF16),
            pltpu.VMEM((n - 1, half, width), BF16),
            pltpu.VMEM((half, width), BF16),
            dma((4,)), dma((chips,)), dma((layers, 9)), dma((chips,)),
            dma((n - 1,)), dma((n - 1,)), dma((n - 1,)), dma((n - 1,)),
        ]
        anyspace = pl.BlockSpec(memory_space=pl.ANY)
        return pl.pallas_call(
            functools.partial(kernel, n),
            out_shape=jax.ShapeDtypeStruct((toks, dim), BF16),
            in_specs=[anyspace] * 14,
            out_specs=anyspace,
            scratch_shapes=scratch,
            compiler_params=pltpu.CompilerParams(collective_id=0, has_side_effects=True, vmem_limit_bytes=60 * 1024 * 1024),
        )(x, lengths.reshape(1, toks), freq, k, v, attn_norm, mlp_norm, w_q, w_k, w_v, w_o, w_gate, w_up, w_down)

    return jax.shard_map(step, mesh=mesh, in_specs=in_specs, out_specs=P("dp", None), check_vma=False)
```
